32 devices in a mesh: frames: 2 (over core), pix: 16 (over z, y, x).
Axes of the slice: x: 2, y: 2, z: 4, core: 2. Of those that a mesh axis runs over, the one named last changes fastest.
Arguments:
- frames: float32 [256, 32768], P('frames', 'pix'), may hold values from -6 to 6
Outputs:
- sketch: float32 [128, 32768], P(None, 'pix')
- projected: float32 [256, 32768], P('frames', 'pix')
The draws below stay inside these ranges and needn't reach their ends.
All inputs are finite; a program needn't handle non-finite values.
Results may differ from the reference program's by a relative error of at most 0.0003.
Values sent between devices are 32-bit elements; how exact they have to be, the bound alone decides.
No kernel may reach another device: no remote copies, remote signals or barrier semaphores. Data moves between devices by JAX's collectives and lax.ppermute only.
A program may use at most 64 MiB of HBM per device.

```python
import jax
import jax.numpy as jnp
from jax import lax

ELL = 128
PIX = 32768
POWER = 1
FRAMES = 256
LEVELS = 1
N_FRAMES = 2


def shard_levels(own_key, dims, split, least, top_value):
    gain = 1.0
    for dim, blocks in split:
        draws = jax.random.uniform(jax.random.fold_in(jax.random.fold_in(own_key, 6), dim), (blocks,), jnp.float32, least / len(split), top_value / len(split))
        gain = gain * jnp.repeat(jnp.exp(draws), dims[dim] // blocks).reshape((-1,) + (1,) * (len(dims) - 1 - dim))
    return gain


def noise(own_key, extent, spread, reach, split=(), kind=jnp.bfloat16):
    array = spread * jax.random.normal(own_key, extent, jnp.float32)
    if split:
        array = array * shard_levels(own_key, extent, split, -0.22, 0.18)
    return jnp.clip(array, -reach, reach).astype(kind)


def setup_inputs(seed: int = 0) -> dict:
    key_of = jax.random.split(jax.random.key(seed), 2)
    return {
        "frames": noise(key_of[0], (FRAMES, PIX), 1.0, 6.0, ((0, 2), (1, 16)), jnp.float32),
    }


def hdot(left, right):
    return jnp.dot(left.astype(jnp.float32), right.astype(jnp.float32), precision=lax.Precision.HIGHEST, preferred_element_type=jnp.float32)

def lower_solve(factor, rhs):
    return lax.linalg.triangular_solve(factor, rhs, left_side=True, lower=True)

def rotation(stacked_gram):
    kept = stacked_gram.shape[0] // 2
    subspace = jnp.eye(2 * kept, kept, dtype=jnp.float32)
    for _ in range(POWER):
        product = hdot(stacked_gram, subspace)
        factor = jnp.linalg.cholesky(hdot(product.T, product))
        subspace = lower_solve(factor, product.T).T
    reduced = hdot(subspace.T, hdot(stacked_gram, subspace))
    root_factor = jnp.linalg.cholesky(reduced)
    delta = jnp.trace(reduced) / kept
    damped = jnp.linalg.cholesky(reduced + delta * jnp.eye(kept, dtype=jnp.float32))
    shrunk = lower_solve(damped, reduced)
    whitened = lower_solve(root_factor, subspace.T)
    mixing = hdot(shrunk.T, whitened)
    return (mixing, hdot(shrunk.T, shrunk))

def merge_pair(lower_rows, lower_gram, upper_rows, upper_gram):
    kept = lower_rows.shape[0]
    cross = hdot(lower_rows, upper_rows.T)
    stacked_gram = jnp.concatenate([jnp.concatenate([lower_gram, cross], axis=1), jnp.concatenate([cross.T, upper_gram], axis=1)], axis=0)
    mixing, new_gram = rotation(stacked_gram)
    merged = hdot(mixing[:, :kept], lower_rows) + hdot(mixing[:, kept:], upper_rows)
    return (merged, new_gram)

def reference(frames):
    sketches = frames.reshape(N_FRAMES, ELL, PIX)
    grams = jax.vmap(lambda rows: hdot(rows, rows.T))(sketches)
    for _ in range(LEVELS):
        sketches, grams = jax.vmap(merge_pair)(sketches[0::2], grams[0::2], sketches[1::2], grams[1::2])
    sketch = sketches[0]
    root_gram = grams[0]
    coeffs = hdot(frames, sketch.T)
    scaling = 4.0 * ELL / (jnp.trace(root_gram) + 1e-06)
    projected = hdot(coeffs, sketch) * scaling
    return (sketch, projected)
```

```python
import jax
import jax.numpy as jnp
from jax import lax
from jax.experimental import pallas as pl
from jax.experimental.pallas import tpu as pltpu
from jax.sharding import PartitionSpec as P

PANEL = 32


def nn(left, right):
    return lax.dot_general(left, right, (((1,), (0,)), ((), ())), precision=lax.Precision.HIGHEST, preferred_element_type=jnp.float32)


def nt(left, right):
    return lax.dot_general(left, right, (((1,), (1,)), ((), ())), precision=lax.Precision.HIGHEST, preferred_element_type=jnp.float32)


def parity(index):
    for shift in (16, 8, 4, 2, 1):
        index = index ^ (index >> shift)
    return index & 1


def half_of(core_axis, axis):
    return lax.axis_index(core_axis) ^ parity(lax.axis_index(axis))


def sum_over(block, axis, core_axis):
    count = lax.axis_size(axis)
    steps = [1 << k for k in range(count.bit_length() - 1)]
    steps = steps[-1:] + steps[:-1]
    for k in range(len(steps)):
        swapped = k ^ 1 if k ^ 1 < len(steps) else k
        route = []
        for core in range(2):
            for i in range(count):
                step = steps[swapped if core ^ parity(i) else k]
                route.append((core * count + i, (1 - core) * count + (i ^ step)))
        block = block + lax.ppermute(block, (core_axis, axis), route)
    return block


def across(block, column):
    return jnp.broadcast_to(block[:, column : column + 1], block.shape)


def down(block, row):
    return jnp.broadcast_to(block[row : row + 1, :], block.shape)


def eliminate(diag, start, rows):
    many = len(diag)
    size = 8 * many
    sub = lax.broadcasted_iota(jnp.int32, diag[0].shape, 0)
    cols = {(c, r): across(diag[r], start + c) for c in range(size) for r in range(c // 8, many)}
    rows = list(rows)
    for j in range(size):
        strip, at = divmod(j, 8)
        inverse = lax.rsqrt(down(cols[j, strip], at))
        low = {r: cols[j, r] * inverse for r in range(strip, many)}
        for c in range(j + 1, size):
            factor = down(low[c // 8], c % 8)
            for r in range(c // 8, many):
                cols[c, r] = cols[c, r] - low[r] * factor
        row = down(rows[strip], at) * inverse
        under = jnp.where(sub > at, low[strip], 0.0)
        rows[strip] = jnp.where(sub == at, row, rows[strip] - under * row)
        for r in range(strip + 1, many):
            rows[r] = rows[r] - low[r] * row
    return rows


def inverse_factors(grams):
    size = grams[0].shape[0]
    column = lax.broadcasted_iota(jnp.int32, (8, size), 1)
    sub = lax.broadcasted_iota(jnp.int32, (8, size), 0)
    done = [[] for _ in grams]
    for start in range(0, size, PANEL):
        for k, gram in enumerate(grams):
            offsets = range(start, start + PANEL, 8)
            mine = [gram[i : i + 8] for i in offsets]
            unit = [(column == sub + i).astype(jnp.float32) for i in offsets]
            if start:
                above = jnp.concatenate(done[k] + [jnp.zeros((size - start, size), jnp.float32)], axis=0)
                low = nt(jnp.concatenate(mine, axis=0), above)
                padded = [jnp.zeros((start, size), jnp.float32), low]
                if size - start - PANEL:
                    padded.append(jnp.zeros((size - start - PANEL, size), jnp.float32))
                square = nt(low, jnp.concatenate(padded, axis=0))
                back = nn(low, above)
                mine = [v - square[8 * i : 8 * i + 8] for i, v in enumerate(mine)]
                unit = [v - back[8 * i : 8 * i + 8] for i, v in enumerate(unit)]
            done[k] += eliminate(mine, start, unit)
    return [jnp.concatenate(d, axis=0) for d in done]


def total(block):
    return jnp.sum(jnp.sum(block, axis=0, keepdims=True), axis=1, keepdims=True)


def transform(lower_gram, cross, upper_gram, is_upper):
    kept = lower_gram.shape[0]
    normal = nt(lower_gram, lower_gram) + nt(cross, cross)
    beside = nn(lower_gram, cross) + nn(cross, upper_gram)
    (inverse,) = inverse_factors([normal])
    basis = nn(inverse, lower_gram), nn(inverse, cross)
    image = nn(inverse, normal), nn(inverse, beside)
    reduced = nt(image[0], basis[0]) + nt(image[1], basis[1])
    delta = total(image[0] * basis[0] + image[1] * basis[1]) / kept
    on_diagonal = lax.broadcasted_iota(jnp.int32, reduced.shape, 0) == lax.broadcasted_iota(jnp.int32, reduced.shape, 1)
    root, damped = inverse_factors([reduced, reduced + jnp.where(on_diagonal, delta, 0.0)])
    shrunk = nt(reduced, damped)
    whitened = nn(root, basis[0]), nn(root, basis[1])
    mixing = nn(shrunk, whitened[0]), nn(shrunk, whitened[1])
    left = jnp.where(is_upper, cross.T, lower_gram)
    right = jnp.where(is_upper, upper_gram, cross)
    scaling = 4.0 * kept / (total(shrunk * shrunk) + 1e-06)
    coeffs = nt(nt(left, whitened[0]) + nt(right, whitened[1]), shrunk) * scaling
    return mixing, coeffs


def split(block):
    high = block.astype(jnp.bfloat16)
    return high, (block - high.astype(jnp.float32)).astype(jnp.bfloat16)


def stacked(block):
    high, low = split(block)
    return jnp.concatenate([high, low], axis=0), high


def product(left, right_high, right_low):
    both, high = left
    rows = high.shape[0]
    out = jnp.dot(both, right_high, preferred_element_type=jnp.float32)
    return out[:rows] + (out[rows:] + jnp.dot(high, right_low, preferred_element_type=jnp.float32))


def positions(size):
    return (lax.broadcasted_iota(jnp.int32, (size, size), axis) for axis in (0, 1))


def own_gram_kernel(own_ref, gram_ref, kept_ref):
    own = own_ref[...]
    kept_ref[...] = own
    gram_ref[...] = nt(own, own)


def pack_kernel(own_ref, other_ref, own_gram_ref, packed_ref):
    kept = own_ref.shape[0]
    is_upper = lax.axis_index("frames") == 1
    is_cross = half_of("frames", "pix") == 0
    own, other = own_ref[...], other_ref[...]
    left = jnp.where(is_cross & ~is_upper, own, other)
    right = jnp.where(is_cross & is_upper, own, other)
    fresh = nt(left, right)
    row, column = positions(kept)
    own_gram = own_gram_ref[...]
    upper_gram = jnp.where(is_upper, own_gram, fresh)
    mixed = jnp.where(row >= column, jnp.where(is_upper, fresh, own_gram), upper_gram)
    packed_ref[:kept] = jnp.where(is_cross, fresh, mixed)
    diagonal = jnp.sum(jnp.where(row == column, upper_gram, 0.0), axis=0, keepdims=True)
    packed_ref[kept:] = jnp.broadcast_to(diagonal, (8, kept))


def unpack(packed):
    kept = packed.shape[1]
    row, column = positions(kept)
    mixed = packed[:kept]
    turned = mixed.T
    lower_gram = jnp.where(row >= column, mixed, turned)
    upper_gram = jnp.where(row < column, mixed, jnp.where(row > column, turned, packed[kept : kept + 1]))
    return lower_gram, upper_gram


def packed_grams(own, other):
    kept, width = own.shape
    whole = pl.BlockSpec(memory_space=pltpu.VMEM)
    grant = pltpu.CompilerParams(vmem_limit_bytes=16 << 20)
    own_gram, own = pl.pallas_call(
        own_gram_kernel,
        in_specs=[whole],
        out_specs=(whole, whole),
        out_shape=(jax.ShapeDtypeStruct((kept, kept), jnp.float32), jax.ShapeDtypeStruct((kept, width), jnp.float32)),
        compiler_params=grant,
        cost_estimate=pl.CostEstimate(flops=12 * kept * kept * width, bytes_accessed=4 * kept * width, transcendentals=0),
    )(own)
    packed = pl.pallas_call(
        pack_kernel,
        in_specs=[whole] * 3,
        out_specs=whole,
        out_shape=jax.ShapeDtypeStruct((kept + 8, kept), jnp.float32),
        compiler_params=grant,
        cost_estimate=pl.CostEstimate(flops=12 * kept * kept * width, bytes_accessed=8 * kept * width, transcendentals=0),
    )(own, other, own_gram)
    return packed, own


def finish_kernel(summed_ref, given_ref, high_ref, low_ref, sketch_ref, projected_ref, sketch_buf, projected_buf, sems):
    kept, width = sketch_buf.shape
    is_upper = lax.axis_index("frames") == 1
    has_cross = half_of("frames", "pix") == 0
    cross = jnp.where(has_cross, summed_ref[:kept], given_ref[:kept])
    lower_gram, upper_gram = unpack(jnp.where(has_cross, given_ref[...], summed_ref[...]))
    (first, second), coeffs = transform(lower_gram, cross, upper_gram, is_upper)
    mixing = stacked(jnp.concatenate([jnp.where(is_upper, second, first), jnp.where(is_upper, first, second)], axis=1))
    coeffs = stacked(coeffs)
    block = min(width, 512)
    copies = []
    for k in range(width // block):
        columns = pl.ds(k * block, block)
        sketch = product(mixing, high_ref[:, columns], low_ref[:, columns])
        sketch_buf[:, columns] = sketch
        copies.append(pltpu.make_async_copy(sketch_buf.at[:, columns], sketch_ref.at[:, columns], sems.at[2 * k]))
        copies[-1].start()
        projected_buf[:, columns] = product(coeffs, *split(sketch))
        copies.append(pltpu.make_async_copy(projected_buf.at[:, columns], projected_ref.at[:, columns], sems.at[2 * k + 1]))
        copies[-1].start()
    for copy in copies:
        copy.wait()


def finish(summed, given, high, low):
    width = high.shape[1]
    kept = high.shape[0] // 2
    whole = pl.BlockSpec(memory_space=pltpu.VMEM)
    return pl.pallas_call(
        finish_kernel,
        in_specs=[whole] * 4,
        out_specs=(pl.BlockSpec(memory_space=pl.ANY),) * 2,
        out_shape=(jax.ShapeDtypeStruct((kept, width), jnp.float32),) * 2,
        scratch_shapes=[pltpu.VMEM((kept, width), jnp.float32)] * 2 + [pltpu.SemaphoreType.DMA((2 * max(1, width // 512),))],
        compiler_params=pltpu.CompilerParams(vmem_limit_bytes=24 << 20),
    )(summed, given, high, low)


def local(frames):
    other = lax.ppermute(frames, "frames", [(0, 1), (1, 0)])
    packed, own = packed_grams(frames, other)
    summed = sum_over(packed, "pix", "frames")
    given = lax.ppermute(summed, "frames", [(0, 1), (1, 0)])
    rows = jnp.concatenate([own, other], axis=0)
    high = lax.reduce_precision(rows, 8, 7)
    low = (rows - high).astype(jnp.bfloat16)
    return finish(summed, given, high.astype(jnp.bfloat16), low)


def solution(mesh):
    count = mesh.shape["pix"]
    if mesh.shape["frames"] != 2 or count & (count - 1):
        raise ValueError("mesh shape")
    return jax.shard_map(
        local,
        mesh=mesh,
        in_specs=(P("frames", "pix"),),
        out_specs=(P(None, "pix"), P("frames", "pix")),
        check_vma=False,
    )
```

```python
import jax
import jax.numpy as jnp
from jax import lax
from jax.experimental import pallas as pl
from jax.experimental.pallas import tpu as pltpu
from jax.sharding import PartitionSpec as P

PANEL = 32


def nn(left, right):
    return lax.dot_general(left, right, (((1,), (0,)), ((), ())), precision=lax.Precision.HIGHEST, preferred_element_type=jnp.float32)


def nt(left, right):
    return lax.dot_general(left, right, (((1,), (1,)), ((), ())), precision=lax.Precision.HIGHEST, preferred_element_type=jnp.float32)


def parity(index):
    for shift in (16, 8, 4, 2, 1):
        index = index ^ (index >> shift)
    return index & 1


def half_of(core_axis, axis):
    return lax.axis_index(core_axis) ^ parity(lax.axis_index(axis))


def sum_over(block, axis, core_axis):
    count = lax.axis_size(axis)
    steps = [1 << k for k in range(count.bit_length() - 1)]
    steps = steps[-1:] + steps[:-1]
    for k in range(len(steps)):
        swapped = k ^ 1 if k ^ 1 < len(steps) else k
        route = []
        for core in range(2):
            for i in range(count):
                step = steps[swapped if core ^ parity(i) else k]
                route.append((core * count + i, (1 - core) * count + (i ^ step)))
        block = block + lax.ppermute(block, (core_axis, axis), route)
    return block


def across(block, column):
    return jnp.broadcast_to(block[:, column : column + 1], block.shape)


def down(block, row):
    return jnp.broadcast_to(block[row : row + 1, :], block.shape)


def eliminate(diag, start, carried, group, ahead):
    many = len(diag)
    size = 8 * many
    sub = lax.broadcasted_iota(jnp.int32, diag[0].shape, 0)
    strips = list(diag)
    carried = [list(rows) for rows in carried]
    cols = {}
    ready = 0
    for j in range(size):
        if j + ahead >= ready and ready < size:
            for c in range(ready, ready + group):
                for r in range(c // 8, many):
                    cols[c, r] = across(strips[r], start + c)
            ready += group
        strip, at = divmod(j, 8)
        inverse = lax.rsqrt(down(cols[j, strip], at))
        low = {r: cols[j, r] * inverse for r in range(strip, many)}
        for c in range(j + 1, ready):
            factor = down(low[c // 8], c % 8)
            for r in range(c // 8, many):
                cols[c, r] = cols[c, r] - low[r] * factor
        under = jnp.where(sub > at, low[strip], 0.0)
        for rows in carried + ([strips] if ready < size else []):
            row = down(rows[strip], at) * inverse
            rows[strip] = jnp.where(sub == at, row, rows[strip] - under * row)
            for r in range(strip + 1, many):
                rows[r] = rows[r] - low[r] * row
    return carried


def inverse_factors(grams, group, ahead):
    size = grams[0].shape[0]
    count, step = size // 8, PANEL // 8
    column = lax.broadcasted_iota(jnp.int32, (8, size), 1)
    sub = lax.broadcasted_iota(jnp.int32, (8, size), 0)
    left = [[gram[8 * i : 8 * i + 8] for i in range(count)] for gram in grams]
    right = [[(column == sub + 8 * i).astype(jnp.float32) for i in range(count)] for _ in grams]
    for first in range(0, count, step):
        rest = first + step
        for a, z in zip(left, right):
            block = a[first:rest]
            if rest == count:
                (z[first:rest],) = eliminate(block, 8 * first, [z[first:rest]], group, ahead)
                continue
            z[first:rest], above = eliminate(block, 8 * first, [z[first:rest], block], group, ahead)
            above = jnp.concatenate(above, axis=0)
            both = jnp.concatenate([above, jnp.concatenate(z[first:rest], axis=0)], axis=1)
            update = nn(above.T[8 * rest :], both)
            for i in range(rest, count):
                rows = slice(8 * (i - rest), 8 * (i - rest) + 8)
                a[i] = a[i] - update[rows, :size]
                z[i] = z[i] - update[rows, size:]
    return [jnp.concatenate(z, axis=0) for z in right]


def total(block):
    return jnp.sum(jnp.sum(block, axis=0, keepdims=True), axis=1, keepdims=True)


def transform(lower_gram, cross, upper_gram, is_upper):
    kept = lower_gram.shape[0]
    normal = nt(lower_gram, lower_gram) + nt(cross, cross)
    beside = nn(lower_gram, cross) + nn(cross, upper_gram)
    (inverse,) = inverse_factors([normal], 16, 6)
    basis = nn(inverse, lower_gram), nn(inverse, cross)
    image = nn(inverse, normal), nn(inverse, beside)
    reduced = nt(image[0], basis[0]) + nt(image[1], basis[1])
    delta = total(image[0] * basis[0] + image[1] * basis[1]) / kept
    on_diagonal = lax.broadcasted_iota(jnp.int32, reduced.shape, 0) == lax.broadcasted_iota(jnp.int32, reduced.shape, 1)
    root, damped = inverse_factors([reduced, reduced + jnp.where(on_diagonal, delta, 0.0)], 8, 4)
    shrunk = nt(reduced, damped)
    whitened = nn(root, basis[0]), nn(root, basis[1])
    mixing = nn(shrunk, whitened[0]), nn(shrunk, whitened[1])
    left = jnp.where(is_upper, cross.T, lower_gram)
    right = jnp.where(is_upper, upper_gram, cross)
    scaling = 4.0 * kept / (total(shrunk * shrunk) + 1e-06)
    coeffs = nt(nt(left, whitened[0]) + nt(right, whitened[1]), shrunk) * scaling
    return mixing, coeffs


def split(block):
    high = block.astype(jnp.bfloat16)
    return high, (block - high.astype(jnp.float32)).astype(jnp.bfloat16)


def stacked(block):
    high, low = split(block)
    return jnp.concatenate([high, low], axis=0), high


def product(left, right_high, right_low):
    both, high = left
    rows = high.shape[0]
    out = jnp.dot(both, right_high, preferred_element_type=jnp.float32)
    return out[:rows] + (out[rows:] + jnp.dot(high, right_low, preferred_element_type=jnp.float32))


def positions(size):
    return (lax.broadcasted_iota(jnp.int32, (size, size), axis) for axis in (0, 1))


def own_gram_kernel(own_ref, gram_ref, kept_ref):
    own = own_ref[...]
    kept_ref[...] = own
    gram_ref[...] = nt(own, own)


def pack_kernel(own_ref, other_ref, own_gram_ref, packed_ref):
    kept = own_ref.shape[0]
    is_upper = lax.axis_index("frames") == 1
    is_cross = half_of("frames", "pix") == 0
    own, other = own_ref[...], other_ref[...]
    left = jnp.where(is_cross & ~is_upper, own, other)
    right = jnp.where(is_cross & is_upper, own, other)
    fresh = nt(left, right)
    row, column = positions(kept)
    own_gram = own_gram_ref[...]
    upper_gram = jnp.where(is_upper, own_gram, fresh)
    mixed = jnp.where(row >= column, jnp.where(is_upper, fresh, own_gram), upper_gram)
    packed_ref[:kept] = jnp.where(is_cross, fresh, mixed)
    diagonal = jnp.sum(jnp.where(row == column, upper_gram, 0.0), axis=0, keepdims=True)
    packed_ref[kept:] = jnp.broadcast_to(diagonal, (8, kept))


def unpack(packed):
    kept = packed.shape[1]
    row, column = positions(kept)
    mixed = packed[:kept]
    turned = mixed.T
    lower_gram = jnp.where(row >= column, mixed, turned)
    upper_gram = jnp.where(row < column, mixed, jnp.where(row > column, turned, packed[kept : kept + 1]))
    return lower_gram, upper_gram


def packed_grams(own, other):
    kept, width = own.shape
    whole = pl.BlockSpec(memory_space=pltpu.VMEM)
    grant = pltpu.CompilerParams(vmem_limit_bytes=16 << 20)
    own_gram, own = pl.pallas_call(
        own_gram_kernel,
        in_specs=[whole],
        out_specs=(whole, whole),
        out_shape=(jax.ShapeDtypeStruct((kept, kept), jnp.float32), jax.ShapeDtypeStruct((kept, width), jnp.float32)),
        compiler_params=grant,
        cost_estimate=pl.CostEstimate(flops=12 * kept * kept * width, bytes_accessed=4 * kept * width, transcendentals=0),
    )(own)
    packed = pl.pallas_call(
        pack_kernel,
        in_specs=[whole] * 3,
        out_specs=whole,
        out_shape=jax.ShapeDtypeStruct((kept + 8, kept), jnp.float32),
        compiler_params=grant,
        cost_estimate=pl.CostEstimate(flops=12 * kept * kept * width, bytes_accessed=8 * kept * width, transcendentals=0),
    )(own, other, own_gram)
    return packed, own


def finish_kernel(summed_ref, given_ref, high_ref, low_ref, sketch_ref, projected_ref, sketch_buf, projected_buf, sems):
    kept, width = sketch_buf.shape
    is_upper = lax.axis_index("frames") == 1
    has_cross = half_of("frames", "pix") == 0
    cross = jnp.where(has_cross, summed_ref[:kept], given_ref[:kept])
    lower_gram, upper_gram = unpack(jnp.where(has_cross, given_ref[...], summed_ref[...]))
    (first, second), coeffs = transform(lower_gram, cross, upper_gram, is_upper)
    mixing = stacked(jnp.concatenate([jnp.where(is_upper, second, first), jnp.where(is_upper, first, second)], axis=1))
    coeffs = stacked(coeffs)
    block = min(width, 512)
    copies = []
    for k in range(width // block):
        columns = pl.ds(k * block, block)
        sketch = product(mixing, high_ref[:, columns], low_ref[:, columns])
        sketch_buf[:, columns] = sketch
        copies.append(pltpu.make_async_copy(sketch_buf.at[:, columns], sketch_ref.at[:, columns], sems.at[2 * k]))
        copies[-1].start()
        projected_buf[:, columns] = product(coeffs, *split(sketch))
        copies.append(pltpu.make_async_copy(projected_buf.at[:, columns], projected_ref.at[:, columns], sems.at[2 * k + 1]))
        copies[-1].start()
    for copy in copies:
        copy.wait()


def finish(summed, given, high, low):
    width = high.shape[1]
    kept = high.shape[0] // 2
    whole = pl.BlockSpec(memory_space=pltpu.VMEM)
    return pl.pallas_call(
        finish_kernel,
        in_specs=[whole] * 4,
        out_specs=(pl.BlockSpec(memory_space=pl.ANY),) * 2,
        out_shape=(jax.ShapeDtypeStruct((kept, width), jnp.float32),) * 2,
        scratch_shapes=[pltpu.VMEM((kept, width), jnp.float32)] * 2 + [pltpu.SemaphoreType.DMA((2 * max(1, width // 512),))],
        compiler_params=pltpu.CompilerParams(vmem_limit_bytes=24 << 20),
    )(summed, given, high, low)


def local(frames):
    other = lax.ppermute(frames, "frames", [(0, 1), (1, 0)])
    packed, own = packed_grams(frames, other)
    summed = sum_over(packed, "pix", "frames")
    given = lax.ppermute(summed, "frames", [(0, 1), (1, 0)])
    rows = jnp.concatenate([own, other], axis=0)
    high = lax.reduce_precision(rows, 8, 7)
    low = (rows - high).astype(jnp.bfloat16)
    return finish(summed, given, high.astype(jnp.bfloat16), low)


def solution(mesh):
    count = mesh.shape["pix"]
    if mesh.shape["frames"] != 2 or count & (count - 1):
        raise ValueError("mesh shape")
    return jax.shard_map(
        local,
        mesh=mesh,
        in_specs=(P("frames", "pix"),),
        out_specs=(P(None, "pix"), P("frames", "pix")),
        check_vma=False,
    )
```

```python
import jax
import jax.numpy as jnp
from jax import lax
from jax.experimental import pallas as pl
from jax.experimental.pallas import tpu as pltpu
from jax.sharding import PartitionSpec as P

PANEL = 32


def nn(left, right):
    return lax.dot_general(left, right, (((1,), (0,)), ((), ())), precision=lax.Precision.HIGHEST, preferred_element_type=jnp.float32)


def nt(left, right):
    return lax.dot_general(left, right, (((1,), (1,)), ((), ())), precision=lax.Precision.HIGHEST, preferred_element_type=jnp.float32)


def split(block):
    high = block.astype(jnp.bfloat16)
    return high, (block - high.astype(jnp.float32)).astype(jnp.bfloat16)


def parts(block, axis):
    return jnp.concatenate(split(block), axis=axis)


def corners(block):
    rows, columns = block.shape[0] // 2, block.shape[1] // 2
    top, bottom = block[:rows], block[rows:]
    return top[:, :columns] + (top[:, columns:] + bottom[:, :columns] + bottom[:, columns:])


def nn_parts(left, right):
    return corners(jnp.dot(parts(left, 0), parts(right, 1), preferred_element_type=jnp.float32))


def nt_high_low(left, right):
    return corners(lax.dot_general(left, right, (((1,), (1,)), ((), ())), preferred_element_type=jnp.float32))


def nt_parts(left, right):
    return nt_high_low(parts(left, 0), parts(right, 0))


def parity(index):
    for shift in (16, 8, 4, 2, 1):
        index = index ^ (index >> shift)
    return index & 1


def half_of(core_axis, axis):
    return lax.axis_index(core_axis) ^ parity(lax.axis_index(axis))


def sum_over(block, axis, core_axis):
    count = lax.axis_size(axis)
    steps = [1 << k for k in range(count.bit_length() - 1)]
    steps = steps[-1:] + steps[:-1]
    for k in range(len(steps)):
        swapped = k ^ 1 if k ^ 1 < len(steps) else k
        route = []
        for core in range(2):
            for i in range(count):
                step = steps[swapped if core ^ parity(i) else k]
                route.append((core * count + i, (1 - core) * count + (i ^ step)))
        block = block + lax.ppermute(block, (core_axis, axis), route)
    return block


def across(block, column):
    return jnp.broadcast_to(block[:, column : column + 1], block.shape)


def down(block, row):
    return jnp.broadcast_to(block[row : row + 1, :], block.shape)


def eliminate(diag, start, carried, group, ahead):
    many = len(diag)
    size = 8 * many
    sub = lax.broadcasted_iota(jnp.int32, diag[0].shape, 0)
    strips = list(diag)
    carried = [list(rows) for rows in carried]
    cols = {}
    ready = 0
    for j in range(size):
        if j + ahead >= ready and ready < size:
            for c in range(ready, ready + group):
                for r in range(c // 8, many):
                    cols[c, r] = across(strips[r], start + c)
            ready += group
        strip, at = divmod(j, 8)
        inverse = lax.rsqrt(down(cols[j, strip], at))
        low = {r: cols[j, r] * inverse for r in range(strip, many)}
        for c in range(j + 1, ready):
            factor = down(low[c // 8], c % 8)
            for r in range(c // 8, many):
                cols[c, r] = cols[c, r] - low[r] * factor
        under = jnp.where(sub > at, low[strip], 0.0)
        for rows in carried + ([strips] if ready < size else []):
            row = down(rows[strip], at) * inverse
            rows[strip] = jnp.where(sub == at, row, rows[strip] - under * row)
            for r in range(strip + 1, many):
                rows[r] = rows[r] - low[r] * row
    return carried


def inverse_factors(grams, group, ahead):
    size = grams[0].shape[0]
    count, step = size // 8, PANEL // 8
    column = lax.broadcasted_iota(jnp.int32, (8, size), 1)
    sub = lax.broadcasted_iota(jnp.int32, (8, size), 0)
    left = [[gram[8 * i : 8 * i + 8] for i in range(count)] for gram in grams]
    right = [[(column == sub + 8 * i).astype(jnp.float32) for i in range(count)] for _ in grams]
    for first in range(0, count, step):
        rest = first + step
        for a, z in zip(left, right):
            block = a[first:rest]
            if rest == count:
                (z[first:rest],) = eliminate(block, 8 * first, [z[first:rest]], group, ahead)
                continue
            z[first:rest], above = eliminate(block, 8 * first, [z[first:rest], block], group, ahead)
            above = jnp.concatenate(above, axis=0)
            both = jnp.concatenate([above, jnp.concatenate(z[first:rest], axis=0)], axis=1)
            update = nn(above.T[8 * rest :], both)
            for i in range(rest, count):
                rows = slice(8 * (i - rest), 8 * (i - rest) + 8)
                a[i] = a[i] - update[rows, :size]
                z[i] = z[i] - update[rows, size:]
    return [jnp.concatenate(z, axis=0) for z in right]


def total(block):
    return jnp.sum(jnp.sum(block, axis=0, keepdims=True), axis=1, keepdims=True)


def transform(lower_gram, cross, upper_gram, is_upper):
    kept = lower_gram.shape[0]
    normal = nt(lower_gram, lower_gram) + nt(cross, cross)
    beside = nn(lower_gram, cross) + nn(cross, upper_gram)
    (inverse,) = inverse_factors([normal], 16, 6)
    basis = nn(inverse, lower_gram), nn(inverse, cross)
    image = nn(inverse, normal), nn(inverse, beside)
    reduced = nt(image[0], basis[0]) + nt(image[1], basis[1])
    delta = total(image[0] * basis[0] + image[1] * basis[1]) / kept
    on_diagonal = lax.broadcasted_iota(jnp.int32, reduced.shape, 0) == lax.broadcasted_iota(jnp.int32, reduced.shape, 1)
    root, damped = inverse_factors([reduced, reduced + jnp.where(on_diagonal, delta, 0.0)], 8, 4)
    shrunk = nt(reduced, damped)
    whitened = nn(root, basis[0]), nn(root, basis[1])
    whitened = jnp.concatenate(whitened, axis=1)
    mixing = nn_parts(shrunk, whitened)
    own_rows = jnp.concatenate([jnp.where(is_upper, cross.T, lower_gram), jnp.where(is_upper, upper_gram, cross)], axis=1)
    scaling = 4.0 * kept / (total(shrunk * shrunk) + 1e-06)
    coeffs = nt_parts(nt_parts(own_rows, whitened), shrunk) * scaling
    return mixing, coeffs


def stacked(block):
    high, low = split(block)
    return jnp.concatenate([high, low], axis=0), high


def product(left, right_high, right_low):
    both, high = left
    rows = high.shape[0]
    out = jnp.dot(both, right_high, preferred_element_type=jnp.float32)
    return out[:rows] + (out[rows:] + jnp.dot(high, right_low, preferred_element_type=jnp.float32))


def positions(size):
    return (lax.broadcasted_iota(jnp.int32, (size, size), axis) for axis in (0, 1))


def own_gram_kernel(own_ref, gram_ref, parts_ref):
    own = parts(own_ref[...], 0)
    parts_ref[...] = own
    gram_ref[...] = nt_high_low(own, own)


def pack_kernel(own_ref, other_ref, own_gram_ref, packed_ref, parts_ref):
    kept = other_ref.shape[0]
    is_upper = lax.axis_index("frames") == 1
    is_cross = half_of("frames", "pix") == 0
    own, other = own_ref[...], parts(other_ref[...], 0)
    parts_ref[...] = other
    left = jnp.where(is_cross & ~is_upper, own, other)
    right = jnp.where(is_cross & is_upper, own, other)
    fresh = nt_high_low(left, right)
    row, column = positions(kept)
    own_gram = own_gram_ref[...]
    upper_gram = jnp.where(is_upper, own_gram, fresh)
    mixed = jnp.where(row >= column, jnp.where(is_upper, fresh, own_gram), upper_gram)
    packed_ref[:kept] = jnp.where(is_cross, fresh, mixed)
    diagonal = jnp.sum(jnp.where(row == column, upper_gram, 0.0), axis=0, keepdims=True)
    packed_ref[kept:] = jnp.broadcast_to(diagonal, (8, kept))


def unpack(packed):
    kept = packed.shape[1]
    row, column = positions(kept)
    mixed = packed[:kept]
    turned = mixed.T
    lower_gram = jnp.where(row >= column, mixed, turned)
    upper_gram = jnp.where(row < column, mixed, jnp.where(row > column, turned, packed[kept : kept + 1]))
    return lower_gram, upper_gram


def packed_grams(own, other):
    kept, width = own.shape
    whole = pl.BlockSpec(memory_space=pltpu.VMEM)
    grant = pltpu.CompilerParams(vmem_limit_bytes=16 << 20)
    cost = pl.CostEstimate(flops=12 * kept * kept * width, bytes_accessed=8 * kept * width, transcendentals=0)
    both = jax.ShapeDtypeStruct((2 * kept, width), jnp.bfloat16)
    own_gram, own = pl.pallas_call(
        own_gram_kernel,
        in_specs=[whole],
        out_specs=(whole, whole),
        out_shape=(jax.ShapeDtypeStruct((kept, kept), jnp.float32), both),
        compiler_params=grant,
        cost_estimate=cost,
    )(own)
    packed, other = pl.pallas_call(
        pack_kernel,
        in_specs=[whole] * 3,
        out_specs=(whole, whole),
        out_shape=(jax.ShapeDtypeStruct((kept + 8, kept), jnp.float32), both),
        compiler_params=grant,
        cost_estimate=cost,
    )(own, other, own_gram)
    return packed, own, other


def finish_kernel(summed_ref, given_ref, own_ref, other_ref, sketch_ref, projected_ref, sketch_buf, projected_buf, sems):
    kept, width = sketch_buf.shape
    is_upper = lax.axis_index("frames") == 1
    has_cross = half_of("frames", "pix") == 0
    cross = jnp.where(has_cross, summed_ref[:kept], given_ref[:kept])
    lower_gram, upper_gram = unpack(jnp.where(has_cross, given_ref[...], summed_ref[...]))
    mixing, coeffs = transform(lower_gram, cross, upper_gram, is_upper)
    first, second = mixing[:, :kept], mixing[:, kept:]
    mixing = stacked(jnp.concatenate([jnp.where(is_upper, second, first), jnp.where(is_upper, first, second)], axis=1))
    coeffs = stacked(coeffs)
    block = min(width, 512)
    copies = []
    for k in range(width // block):
        columns = pl.ds(k * block, block)
        high = jnp.concatenate([own_ref[:kept, columns], other_ref[:kept, columns]], axis=0)
        low = jnp.concatenate([own_ref[kept:, columns], other_ref[kept:, columns]], axis=0)
        sketch = product(mixing, high, low)
        sketch_buf[:, columns] = sketch
        copies.append(pltpu.make_async_copy(sketch_buf.at[:, columns], sketch_ref.at[:, columns], sems.at[2 * k]))
        copies[-1].start()
        projected_buf[:, columns] = product(coeffs, *split(sketch))
        copies.append(pltpu.make_async_copy(projected_buf.at[:, columns], projected_ref.at[:, columns], sems.at[2 * k + 1]))
        copies[-1].start()
    for copy in copies:
        copy.wait()


def finish(summed, given, own, other):
    kept, width = own.shape[0] // 2, own.shape[1]
    whole = pl.BlockSpec(memory_space=pltpu.VMEM)
    return pl.pallas_call(
        finish_kernel,
        in_specs=[whole] * 4,
        out_specs=(pl.BlockSpec(memory_space=pl.ANY),) * 2,
        out_shape=(jax.ShapeDtypeStruct((kept, width), jnp.float32),) * 2,
        scratch_shapes=[pltpu.VMEM((kept, width), jnp.float32)] * 2 + [pltpu.SemaphoreType.DMA((2 * max(1, width // 512),))],
        compiler_params=pltpu.CompilerParams(vmem_limit_bytes=24 << 20),
    )(summed, given, own, other)


def local(frames):
    other = lax.ppermute(frames, "frames", [(0, 1), (1, 0)])
    packed, own, other = packed_grams(frames, other)
    summed = sum_over(packed, "pix", "frames")
    given = lax.ppermute(summed, "frames", [(0, 1), (1, 0)])
    return finish(summed, given, own, other)


def solution(mesh):
    count = mesh.shape["pix"]
    if mesh.shape["frames"] != 2 or count & (count - 1):
        raise ValueError("mesh shape")
    return jax.shard_map(
        local,
        mesh=mesh,
        in_specs=(P("frames", "pix"),),
        out_specs=(P(None, "pix"), P("frames", "pix")),
        check_vma=False,
    )
```

```python
import jax
import jax.numpy as jnp
from jax import lax
from jax.experimental import pallas as pl
from jax.experimental.pallas import tpu as pltpu
from jax.sharding import PartitionSpec as P

def nn(left, right):
    return lax.dot_general(left, right, (((1,), (0,)), ((), ())), precision=lax.Precision.HIGHEST, preferred_element_type=jnp.float32)


def nt(left, right):
    return lax.dot_general(left, right, (((1,), (1,)), ((), ())), precision=lax.Precision.HIGHEST, preferred_element_type=jnp.float32)


def split(block):
    high = block.astype(jnp.bfloat16)
    return high, (block - high.astype(jnp.float32)).astype(jnp.bfloat16)


def parts(block, axis):
    return jnp.concatenate(split(block), axis=axis)


def corners(block):
    rows, columns = block.shape[0] // 2, block.shape[1] // 2
    top, bottom = block[:rows], block[rows:]
    return top[:, :columns] + (top[:, columns:] + bottom[:, :columns] + bottom[:, columns:])


def nn_parts(left, right):
    return corners(jnp.dot(parts(left, 0), parts(right, 1), preferred_element_type=jnp.float32))


def nt_high_low(left, right):
    return corners(lax.dot_general(left, right, (((1,), (1,)), ((), ())), preferred_element_type=jnp.float32))


def nt_parts(left, right):
    return nt_high_low(parts(left, 0), parts(right, 0))


def parity(index):
    for shift in (16, 8, 4, 2, 1):
        index = index ^ (index >> shift)
    return index & 1


def half_of(core_axis, axis):
    return lax.axis_index(core_axis) ^ parity(lax.axis_index(axis))


def sum_over(block, axis, core_axis):
    count = lax.axis_size(axis)
    steps = [1 << k for k in range(count.bit_length() - 1)]
    steps = steps[-1:] + steps[:-1]
    for k in range(len(steps)):
        swapped = k ^ 1 if k ^ 1 < len(steps) else k
        route = []
        for core in range(2):
            for i in range(count):
                step = steps[swapped if core ^ parity(i) else k]
                route.append((core * count + i, (1 - core) * count + (i ^ step)))
        block = block + lax.ppermute(block, (core_axis, axis), route)
    return block


def across(block, column):
    return jnp.broadcast_to(block[:, column : column + 1], block.shape)


def down(block, row):
    return jnp.broadcast_to(block[row : row + 1, :], block.shape)


def eliminate(diag, start, carried, group, ahead):
    many = len(diag)
    size = 8 * many
    sub = lax.broadcasted_iota(jnp.int32, diag[0].shape, 0)
    strips = list(diag)
    carried = [list(rows) for rows in carried]
    cols = {}
    ready = 0
    for j in range(size):
        if j + ahead >= ready and ready < size:
            for c in range(ready, ready + group):
                for r in range(c // 8, many):
                    cols[c, r] = across(strips[r], start + c)
            ready += group
        strip, at = divmod(j, 8)
        inverse = lax.rsqrt(down(cols[j, strip], at))
        low = {r: cols[j, r] * inverse for r in range(strip, many)}
        for c in range(j + 1, ready):
            factor = down(low[c // 8], c % 8)
            for r in range(c // 8, many):
                cols[c, r] = cols[c, r] - low[r] * factor
        under = jnp.where(sub > at, low[strip], 0.0)
        for rows in carried + ([strips] if ready < size else []):
            row = down(rows[strip], at) * inverse
            rows[strip] = jnp.where(sub == at, row, rows[strip] - under * row)
            for r in range(strip + 1, many):
                rows[r] = rows[r] - low[r] * row
    return carried


def inverse_factors(grams, panel, group, ahead):
    size = grams[0].shape[0]
    count, step = size // 8, panel // 8
    column = lax.broadcasted_iota(jnp.int32, (8, size), 1)
    sub = lax.broadcasted_iota(jnp.int32, (8, size), 0)
    left = [[gram[8 * i : 8 * i + 8] for i in range(count)] for gram in grams]
    right = [[(column == sub + 8 * i).astype(jnp.float32) for i in range(count)] for _ in grams]
    for first in range(0, count, step):
        rest = min(first + step, count)
        for a, z in zip(left, right):
            block = a[first:rest]
            if rest == count:
                (z[first:rest],) = eliminate(block, 8 * first, [z[first:rest]], group, ahead)
                continue
            z[first:rest], above = eliminate(block, 8 * first, [z[first:rest], block], group, ahead)
            above = jnp.concatenate(above, axis=0)
            both = jnp.concatenate([above, jnp.concatenate(z[first:rest], axis=0)], axis=1)
            update = nn(above.T[8 * rest :], both)
            for i in range(rest, count):
                rows = slice(8 * (i - rest), 8 * (i - rest) + 8)
                a[i] = a[i] - update[rows, :size]
                z[i] = z[i] - update[rows, size:]
    return [jnp.concatenate(z, axis=0) for z in right]


def total(block):
    return jnp.sum(jnp.sum(block, axis=0, keepdims=True), axis=1, keepdims=True)


def transform(lower_gram, cross, upper_gram, is_upper):
    kept = lower_gram.shape[0]
    upper_rows = jnp.concatenate([lower_gram, cross], axis=1)
    normal = nt(upper_rows, upper_rows)
    beside = nn(upper_rows, jnp.concatenate([cross, upper_gram], axis=0))
    (inverse,) = inverse_factors([normal], 48, 8, 4)
    turned = nn(inverse, jnp.concatenate([upper_rows, normal, beside], axis=1))
    basis, image = turned[:, : 2 * kept], turned[:, 2 * kept :]
    reduced = nt(image, basis)
    delta = total(image * basis) / kept
    on_diagonal = lax.broadcasted_iota(jnp.int32, reduced.shape, 0) == lax.broadcasted_iota(jnp.int32, reduced.shape, 1)
    root, damped = inverse_factors([reduced, reduced + jnp.where(on_diagonal, delta, 0.0)], 32, 8, 4)
    shrunk = nt(reduced, damped)
    whitened = nn(root, basis)
    mixing = nn_parts(shrunk, whitened)
    own_rows = jnp.concatenate([jnp.where(is_upper, cross.T, lower_gram), jnp.where(is_upper, upper_gram, cross)], axis=1)
    scaling = 4.0 * kept / (total(shrunk * shrunk) + 1e-06)
    coeffs = nt_parts(nt_parts(own_rows, whitened), shrunk) * scaling
    return mixing, coeffs


def stacked(block):
    high, low = split(block)
    return jnp.concatenate([high, low], axis=0), high


def product(left, right_high, right_low):
    both, high = left
    rows = high.shape[0]
    out = jnp.dot(both, right_high, preferred_element_type=jnp.float32)
    return out[:rows] + (out[rows:] + jnp.dot(high, right_low, preferred_element_type=jnp.float32))


def positions(size):
    return (lax.broadcasted_iota(jnp.int32, (size, size), axis) for axis in (0, 1))


def own_gram_kernel(own_ref, gram_ref, parts_ref):
    own = parts(own_ref[...], 0)
    parts_ref[...] = own
    gram_ref[...] = nt_high_low(own, own)


def pack_kernel(own_ref, other_ref, own_gram_ref, packed_ref, parts_ref):
    kept = other_ref.shape[0]
    is_upper = lax.axis_index("frames") == 1
    is_cross = half_of("frames", "pix") == 0
    own, other = own_ref[...], parts(other_ref[...], 0)
    parts_ref[...] = other
    left = jnp.where(is_cross & ~is_upper, own, other)
    right = jnp.where(is_cross & is_upper, own, other)
    fresh = nt_high_low(left, right)
    row, column = positions(kept)
    own_gram = own_gram_ref[...]
    upper_gram = jnp.where(is_upper, own_gram, fresh)
    mixed = jnp.where(row >= column, jnp.where(is_upper, fresh, own_gram), upper_gram)
    packed_ref[:kept] = jnp.where(is_cross, fresh, mixed)
    diagonal = jnp.sum(jnp.where(row == column, upper_gram, 0.0), axis=0, keepdims=True)
    packed_ref[kept:] = jnp.broadcast_to(diagonal, (8, kept))


def unpack(packed):
    kept = packed.shape[1]
    row, column = positions(kept)
    mixed = packed[:kept]
    turned = mixed.T
    lower_gram = jnp.where(row >= column, mixed, turned)
    upper_gram = jnp.where(row < column, mixed, jnp.where(row > column, turned, packed[kept : kept + 1]))
    return lower_gram, upper_gram


def packed_grams(own, other):
    kept, width = own.shape
    whole = pl.BlockSpec(memory_space=pltpu.VMEM)
    grant = pltpu.CompilerParams(vmem_limit_bytes=16 << 20)
    cost = pl.CostEstimate(flops=12 * kept * kept * width, bytes_accessed=8 * kept * width, transcendentals=0)
    both = jax.ShapeDtypeStruct((2 * kept, width), jnp.bfloat16)
    own_gram, own = pl.pallas_call(
        own_gram_kernel,
        in_specs=[whole],
        out_specs=(whole, whole),
        out_shape=(jax.ShapeDtypeStruct((kept, kept), jnp.float32), both),
        compiler_params=grant,
        cost_estimate=cost,
    )(own)
    packed, other = pl.pallas_call(
        pack_kernel,
        in_specs=[whole] * 3,
        out_specs=(whole, whole),
        out_shape=(jax.ShapeDtypeStruct((kept + 8, kept), jnp.float32), both),
        compiler_params=grant,
        cost_estimate=cost,
    )(own, other, own_gram)
    return packed, own, other


def finish_kernel(summed_ref, given_ref, own_ref, other_ref, sketch_ref, projected_ref, sketch_buf, projected_buf, sems):
    kept, width = sketch_buf.shape
    is_upper = lax.axis_index("frames") == 1
    has_cross = half_of("frames", "pix") == 0
    cross = jnp.where(has_cross, summed_ref[:kept], given_ref[:kept])
    lower_gram, upper_gram = unpack(jnp.where(has_cross, given_ref[...], summed_ref[...]))
    mixing, coeffs = transform(lower_gram, cross, upper_gram, is_upper)
    first, second = mixing[:, :kept], mixing[:, kept:]
    mixing = stacked(jnp.concatenate([jnp.where(is_upper, second, first), jnp.where(is_upper, first, second)], axis=1))
    coeffs = stacked(coeffs)
    block = min(width, 1024)
    copies = []
    for k in range(width // block):
        columns = pl.ds(k * block, block)
        high = jnp.concatenate([own_ref[:kept, columns], other_ref[:kept, columns]], axis=0)
        low = jnp.concatenate([own_ref[kept:, columns], other_ref[kept:, columns]], axis=0)
        sketch = product(mixing, high, low)
        sketch_buf[:, columns] = sketch
        copies.append(pltpu.make_async_copy(sketch_buf.at[:, columns], sketch_ref.at[:, columns], sems.at[2 * k]))
        copies[-1].start()
        projected_buf[:, columns] = product(coeffs, *split(sketch))
        copies.append(pltpu.make_async_copy(projected_buf.at[:, columns], projected_ref.at[:, columns], sems.at[2 * k + 1]))
        copies[-1].start()
    for copy in copies:
        copy.wait()


def finish(summed, given, own, other):
    kept, width = own.shape[0] // 2, own.shape[1]
    whole = pl.BlockSpec(memory_space=pltpu.VMEM)
    return pl.pallas_call(
        finish_kernel,
        in_specs=[whole] * 4,
        out_specs=(pl.BlockSpec(memory_space=pl.ANY),) * 2,
        out_shape=(jax.ShapeDtypeStruct((kept, width), jnp.float32),) * 2,
        scratch_shapes=[pltpu.VMEM((kept, width), jnp.float32)] * 2 + [pltpu.SemaphoreType.DMA((2 * max(1, width // 1024),))],
        compiler_params=pltpu.CompilerParams(vmem_limit_bytes=24 << 20),
    )(summed, given, own, other)


def local(frames):
    other = lax.ppermute(frames, "frames", [(0, 1), (1, 0)])
    packed, own, other = packed_grams(frames, other)
    summed = sum_over(packed, "pix", "frames")
    given = lax.ppermute(summed, "frames", [(0, 1), (1, 0)])
    return finish(summed, given, own, other)


def solution(mesh):
    count = mesh.shape["pix"]
    if mesh.shape["frames"] != 2 or count & (count - 1):
        raise ValueError("mesh shape")
    return jax.shard_map(
        local,
        mesh=mesh,
        in_specs=(P("frames", "pix"),),
        out_specs=(P(None, "pix"), P("frames", "pix")),
        check_vma=False,
    )
```

```python
import jax
import jax.numpy as jnp
from jax import lax
from jax.experimental import pallas as pl
from jax.experimental.pallas import tpu as pltpu
from jax.sharding import PartitionSpec as P

PIECES = 2


def nn(left, right):
    return lax.dot_general(left, right, (((1,), (0,)), ((), ())), precision=lax.Precision.HIGHEST, preferred_element_type=jnp.float32)


def nt(left, right):
    return lax.dot_general(left, right, (((1,), (1,)), ((), ())), precision=lax.Precision.HIGHEST, preferred_element_type=jnp.float32)


def split(block):
    high = block.astype(jnp.bfloat16)
    return high, (block - high.astype(jnp.float32)).astype(jnp.bfloat16)


def parts(block, axis):
    return jnp.concatenate(split(block), axis=axis)


def corners(block):
    rows, columns = block.shape[0] // 2, block.shape[1] // 2
    top, bottom = block[:rows], block[rows:]
    return top[:, :columns] + (top[:, columns:] + bottom[:, :columns] + bottom[:, columns:])


def nn_parts(left, right):
    return corners(jnp.dot(parts(left, 0), parts(right, 1), preferred_element_type=jnp.float32))


def nt_high_low(left, right):
    return corners(lax.dot_general(left, right, (((1,), (1,)), ((), ())), preferred_element_type=jnp.float32))


def nt_parts(left, right):
    return nt_high_low(parts(left, 0), parts(right, 0))


def parity(index):
    for shift in (16, 8, 4, 2, 1):
        index = index ^ (index >> shift)
    return index & 1


def half_of(core_axis, axis):
    return lax.axis_index(core_axis) ^ parity(lax.axis_index(axis))


def sum_over(block, axis, core_axis):
    count = lax.axis_size(axis)
    steps = [1 << k for k in range(count.bit_length() - 1)]
    steps = steps[-1:] + steps[:-1]
    for k in range(len(steps)):
        swapped = k ^ 1 if k ^ 1 < len(steps) else k
        route = []
        for core in range(2):
            for i in range(count):
                step = steps[swapped if core ^ parity(i) else k]
                route.append((core * count + i, (1 - core) * count + (i ^ step)))
        block = block + lax.ppermute(block, (core_axis, axis), route)
    return block


def across(block, column):
    return jnp.broadcast_to(block[:, column : column + 1], block.shape)


def down(block, row):
    return jnp.broadcast_to(block[row : row + 1, :], block.shape)


def eliminate(diag, start, carried, group, ahead):
    many = len(diag)
    size = 8 * many
    sub = lax.broadcasted_iota(jnp.int32, diag[0].shape, 0)
    strips = list(diag)
    carried = [list(rows) for rows in carried]
    cols = {}
    ready = 0
    for j in range(size):
        if j + ahead >= ready and ready < size:
            for c in range(ready, ready + group):
                for r in range(c // 8, many):
                    cols[c, r] = across(strips[r], start + c)
            ready += group
        strip, at = divmod(j, 8)
        inverse = lax.rsqrt(down(cols[j, strip], at))
        low = {r: cols[j, r] * inverse for r in range(strip, many)}
        for c in range(j + 1, ready):
            factor = down(low[c // 8], c % 8)
            for r in range(c // 8, many):
                cols[c, r] = cols[c, r] - low[r] * factor
        under = jnp.where(sub > at, low[strip], 0.0)
        for rows in carried + ([strips] if ready < size else []):
            row = down(rows[strip], at) * inverse
            rows[strip] = jnp.where(sub == at, row, rows[strip] - under * row)
            for r in range(strip + 1, many):
                rows[r] = rows[r] - low[r] * row
    return carried


def inverse_factors(grams, panel, group, ahead):
    size = grams[0].shape[0]
    count, step = size // 8, panel // 8
    column = lax.broadcasted_iota(jnp.int32, (8, size), 1)
    sub = lax.broadcasted_iota(jnp.int32, (8, size), 0)
    left = [[gram[8 * i : 8 * i + 8] for i in range(count)] for gram in grams]
    right = [[(column == sub + 8 * i).astype(jnp.float32) for i in range(count)] for _ in grams]
    for first in range(0, count, step):
        rest = min(first + step, count)
        for a, z in zip(left, right):
            block = a[first:rest]
            if rest == count:
                (z[first:rest],) = eliminate(block, 8 * first, [z[first:rest]], group, ahead)
                continue
            z[first:rest], above = eliminate(block, 8 * first, [z[first:rest], block], group, ahead)
            above = jnp.concatenate(above, axis=0)
            both = jnp.concatenate([above, jnp.concatenate(z[first:rest], axis=0)], axis=1)
            turned = above.T
            soon = min(rest + step, count)
            for low, high in ((rest, soon), (soon, count)):
                if low == high:
                    continue
                update = nn(turned[8 * low : 8 * high], both)
                for i in range(low, high):
                    rows = slice(8 * (i - low), 8 * (i - low) + 8)
                    a[i] = a[i] - update[rows, :size]
                    z[i] = z[i] - update[rows, size:]
    return [jnp.concatenate(z, axis=0) for z in right]


def total(block):
    return jnp.sum(jnp.sum(block, axis=0, keepdims=True), axis=1, keepdims=True)


def transform(lower_gram, cross, upper_gram, is_upper):
    kept = lower_gram.shape[0]
    upper_rows = jnp.concatenate([lower_gram, cross], axis=1)
    normal = nt(upper_rows, upper_rows)
    beside = nn(upper_rows, jnp.concatenate([cross, upper_gram], axis=0))
    (inverse,) = inverse_factors([normal], 48, 8, 4)
    turned = nn(inverse, jnp.concatenate([upper_rows, normal, beside], axis=1))
    basis, image = turned[:, : 2 * kept], turned[:, 2 * kept :]
    reduced = nt(image, basis)
    delta = total(image * basis) / kept
    on_diagonal = lax.broadcasted_iota(jnp.int32, reduced.shape, 0) == lax.broadcasted_iota(jnp.int32, reduced.shape, 1)
    root, damped = inverse_factors([reduced, reduced + jnp.where(on_diagonal, delta, 0.0)], 32, 8, 4)
    shrunk = nt_parts(reduced, damped)
    whitened = nn_parts(root, basis)
    mixing = nn_parts(shrunk, whitened)
    own_rows = jnp.concatenate([jnp.where(is_upper, cross.T, lower_gram), jnp.where(is_upper, upper_gram, cross)], axis=1)
    scaling = 4.0 * kept / (total(shrunk * shrunk) + 1e-06)
    coeffs = nt_parts(nt_parts(own_rows, whitened), shrunk) * scaling
    return mixing, coeffs


def stacked(block):
    high, low = split(block)
    return jnp.concatenate([high, low], axis=0), high


def product(left, right_high, right_low):
    both, high = left
    rows = high.shape[0]
    out = jnp.dot(both, right_high, preferred_element_type=jnp.float32)
    return out[:rows] + (out[rows:] + jnp.dot(high, right_low, preferred_element_type=jnp.float32))


def positions(size):
    return (lax.broadcasted_iota(jnp.int32, (size, size), axis) for axis in (0, 1))


def own_gram_kernel(own_ref, gram_ref, parts_ref):
    own = parts(own_ref[...], 0)
    parts_ref[...] = own
    gram_ref[...] = nt_high_low(own, own)


def pack_kernel(own_ref, other_ref, own_gram_ref, packed_ref, parts_ref):
    kept = other_ref.shape[0]
    is_upper = lax.axis_index("frames") == 1
    is_cross = half_of("frames", "pix") == 0
    own, other = own_ref[...], parts(other_ref[...], 0)
    parts_ref[...] = other
    left = jnp.where(is_cross & ~is_upper, own, other)
    right = jnp.where(is_cross & is_upper, own, other)
    fresh = nt_high_low(left, right)
    row, column = positions(kept)
    own_gram = own_gram_ref[...]
    upper_gram = jnp.where(is_upper, own_gram, fresh)
    mixed = jnp.where(row >= column, jnp.where(is_upper, fresh, own_gram), upper_gram)
    packed_ref[:kept] = jnp.where(is_cross, fresh, mixed)
    diagonal = jnp.sum(jnp.where(row == column, upper_gram, 0.0), axis=0, keepdims=True)
    packed_ref[kept:] = jnp.broadcast_to(diagonal, (8, kept))


def unpack(packed):
    kept = packed.shape[1]
    row, column = positions(kept)
    mixed = packed[:kept]
    turned = mixed.T
    lower_gram = jnp.where(row >= column, mixed, turned)
    upper_gram = jnp.where(row < column, mixed, jnp.where(row > column, turned, packed[kept : kept + 1]))
    return lower_gram, upper_gram


def packed_grams(own, other):
    kept, width = own.shape
    whole = pl.BlockSpec(memory_space=pltpu.VMEM)
    grant = pltpu.CompilerParams(vmem_limit_bytes=16 << 20)
    cost = pl.CostEstimate(flops=12 * kept * kept * width, bytes_accessed=8 * kept * width, transcendentals=0)
    both = jax.ShapeDtypeStruct((2 * kept, width), jnp.bfloat16)
    own_gram, own = pl.pallas_call(
        own_gram_kernel,
        in_specs=[whole],
        out_specs=(whole, whole),
        out_shape=(jax.ShapeDtypeStruct((kept, kept), jnp.float32), both),
        compiler_params=grant,
        cost_estimate=cost,
    )(own)
    packed, other = pl.pallas_call(
        pack_kernel,
        in_specs=[whole] * 3,
        out_specs=(whole, whole),
        out_shape=(jax.ShapeDtypeStruct((kept + 8, kept), jnp.float32), both),
        compiler_params=grant,
        cost_estimate=cost,
    )(own, other, own_gram)
    return packed, own, other


def finish_kernel(summed_ref, given_ref, own_ref, other_ref, sketch_ref, projected_ref, sketch_buf, projected_buf, sems):
    kept, width = sketch_buf.shape
    is_upper = lax.axis_index("frames") == 1
    has_cross = half_of("frames", "pix") == 0
    cross = jnp.where(has_cross, summed_ref[:kept], given_ref[:kept])
    lower_gram, upper_gram = unpack(jnp.where(has_cross, given_ref[...], summed_ref[...]))
    mixing, coeffs = transform(lower_gram, cross, upper_gram, is_upper)
    first, second = mixing[:, :kept], mixing[:, kept:]
    mixing = stacked(jnp.concatenate([jnp.where(is_upper, second, first), jnp.where(is_upper, first, second)], axis=1))
    coeffs = stacked(coeffs)
    high = jnp.concatenate([own_ref[:kept], other_ref[:kept]], axis=0)
    low = jnp.concatenate([own_ref[kept:], other_ref[kept:]], axis=0)
    sketch = product(mixing, high, low)
    sketch_buf[...] = sketch
    copies = [pltpu.make_async_copy(sketch_buf, sketch_ref, sems.at[0])]
    copies[0].start()
    block = width // PIECES
    for k in range(PIECES):
        columns = slice(k * block, (k + 1) * block)
        projected_buf[:, columns] = product(coeffs, *split(sketch[:, columns]))
        copies.append(pltpu.make_async_copy(projected_buf.at[:, columns], projected_ref.at[:, columns], sems.at[k + 1]))
        copies[-1].start()
    for copy in copies:
        copy.wait()


def finish(summed, given, own, other):
    kept, width = own.shape[0] // 2, own.shape[1]
    whole = pl.BlockSpec(memory_space=pltpu.VMEM)
    return pl.pallas_call(
        finish_kernel,
        in_specs=[whole] * 4,
        out_specs=(pl.BlockSpec(memory_space=pl.ANY),) * 2,
        out_shape=(jax.ShapeDtypeStruct((kept, width), jnp.float32),) * 2,
        scratch_shapes=[pltpu.VMEM((kept, width), jnp.float32)] * 2 + [pltpu.SemaphoreType.DMA((PIECES + 1,))],
        compiler_params=pltpu.CompilerParams(vmem_limit_bytes=24 << 20),
    )(summed, given, own, other)


def local(frames):
    other = lax.ppermute(frames, "frames", [(0, 1), (1, 0)])
    packed, own, other = packed_grams(frames, other)
    summed = sum_over(packed, "pix", "frames")
    given = lax.ppermute(summed, "frames", [(0, 1), (1, 0)])
    return finish(summed, given, own, other)


def solution(mesh):
    count = mesh.shape["pix"]
    if mesh.shape["frames"] != 2 or count & (count - 1):
        raise ValueError("mesh shape")
    return jax.shard_map(
        local,
        mesh=mesh,
        in_specs=(P("frames", "pix"),),
        out_specs=(P(None, "pix"), P("frames", "pix")),
        check_vma=False,
    )
```
